16 devices in a mesh: rep: 4 (over y, z, core), dp: 4 (over x).
Axes of the slice: x: 4, y: 2, z: 1, core: 2. Of those that a mesh axis runs over, the one named last changes fastest.
The devices are a block of a 4x4x8 slice.
Arguments:
- x: bfloat16 [16, 4096, 1024], P(('rep', 'dp')), parts along dimension 0
- dy: bfloat16 [16, 4096, 1024], P(('rep', 'dp')), parts along dimension 0
- w_gate: bfloat16 [2, 1024, 3200], P(None, 'dp')
- w_up: bfloat16 [2, 1024, 3200], P(None, 'dp')
- w_down: bfloat16 [2, 3200, 1024], P(None, 'dp')
- m_w_gate: float32 [2, 1024, 3200], P(None, 'dp')
- m_w_up: float32 [2, 1024, 3200], P(None, 'dp')
- m_w_down: float32 [2, 3200, 1024], P(None, 'dp')
- v_w_gate: float32 [2, 1024, 3200], P(None, 'dp')
- v_w_up: float32 [2, 1024, 3200], P(None, 'dp')
- v_w_down: float32 [2, 3200, 1024], P(None, 'dp')
Outputs:
- output 1: bfloat16 [8, 1024, 3200], P('rep', 'dp'), parts along dimension 0
- output 2: bfloat16 [8, 1024, 3200], P('rep', 'dp'), parts along dimension 0
- output 3: bfloat16 [8, 3200, 1024], P('rep', 'dp'), parts along dimension 0
- output 4: float32 [8, 1024, 3200], P('rep', 'dp'), parts along dimension 0
- output 5: float32 [8, 1024, 3200], P('rep', 'dp'), parts along dimension 0
- output 6: float32 [8, 3200, 1024], P('rep', 'dp'), parts along dimension 0
- output 7: float32 [8, 1024, 3200], P('rep', 'dp'), parts along dimension 0
- output 8: float32 [8, 1024, 3200], P('rep', 'dp'), parts along dimension 0
- output 9: float32 [8, 3200, 1024], P('rep', 'dp'), parts along dimension 0
There are 4 independent parts. The reference program is written for one: setup_inputs(seed, part) draws one part's arguments, and reference() takes and returns one part's arrays. A program takes and returns all parts, laid end to end along the dimension named above; an argument that names none is the same for every part.
All inputs are finite; a program needn't handle non-finite values.
Results may differ from the reference program's by a relative error of at most 0.022.
Values are sent between devices in bfloat16 or wider.
A program may use at most 768 MiB of HBM per device.

```python
import jax
import jax.numpy as jnp
from jax import lax

SEQUENCES = 4
TOKENS = 4096
D = 1024
FF = 3200
LAYERS = 2
NAMES = ("w_gate", "w_up", "w_down")
SHAPES = {"w_gate": (LAYERS, D, FF), "w_up": (LAYERS, D, FF), "w_down": (LAYERS, FF, D)}


def bump(key, n, height):
    away = (jnp.arange(n, dtype=jnp.int32) - jax.random.randint(key, (), 0, n, jnp.int32)) % n
    return jnp.where(away < n // 8, height, 1.0)


def together(key, own, strength):
    shared = jax.random.normal(key, own.shape[1:], jnp.float32)
    return (own + strength * shared) * lax.rsqrt(1 + strength * strength)


def setup_inputs(seed: int = 0, part: int = 0) -> dict:
    kx, kdy, ka, kb, kz, kf, kh, kl, *keys = jax.random.split(jax.random.key(seed), 8 + 3 * len(NAMES))
    kx, kdy, ka, kb = (jax.random.fold_in(k, part) for k in (kx, kdy, ka, kb))
    kw, km, kv = (keys[i::3] for i in range(3))
    shape = (SEQUENCES, TOKENS, D)
    much_x, much_dy = jax.random.uniform(kz, (2,), jnp.float32, 0.0, 1.0)
    loud = 2.0 ** jax.random.uniform(jax.random.fold_in(kz, 1), (), jnp.float32, -1.0, 2.0)
    layers = 2.0 ** jax.random.uniform(kl, (LAYERS, 1, 1), jnp.float32, -1.0, 1.0)
    x = together(ka, jax.random.normal(kx, shape, jnp.float32), much_x) * bump(kf, D, 4.0)
    dy = together(kb, jax.random.normal(kdy, shape, jnp.float32), much_dy)
    drawn = {"x": x.astype(jnp.bfloat16), "dy": (loud * dy * (SEQUENCES * TOKENS) ** -0.5).astype(jnp.bfloat16)}
    for key, name in zip(kw, NAMES, strict=True):
        w = jax.random.normal(key, SHAPES[name], jnp.float32) * SHAPES[name][1] ** -0.5
        drawn[name] = (w * {"w_gate": 1.0, "w_up": bump(kh, FF, 4.0), "w_down": layers}[name]).astype(jnp.bfloat16)
    for key, name in zip(km, NAMES, strict=True):
        drawn[f"m_{name}"] = 0.1 * jax.random.normal(key, SHAPES[name], jnp.float32)
    for key, name in zip(kv, NAMES, strict=True):
        drawn[f"v_{name}"] = jax.random.uniform(key, SHAPES[name], jnp.float32, 0.005, 0.015)
    return drawn


def matmul(a, w):
    return jnp.dot(a, w, preferred_element_type=jnp.float32).astype(jnp.bfloat16)


def normed(h):
    wide = h.astype(jnp.float32)
    scale = lax.rsqrt(jnp.mean(wide**2, -1, keepdims=True) + 1e-6)
    return (wide * scale).astype(jnp.bfloat16)


def layer(h, w):
    a = normed(h)
    gate = jnp.dot(a, w["w_gate"], preferred_element_type=jnp.float32)
    up = jnp.dot(a, w["w_up"], preferred_element_type=jnp.float32)
    return h + matmul((jax.nn.silu(gate) * up).astype(jnp.bfloat16), w["w_down"])


def adamw(w, m, v, g):
    m = 0.9 * m + 0.1 * g
    v = 0.95 * v + 0.05 * g * g
    step = m * lax.rsqrt(v + 1e-8) + 0.1 * w
    return (w - 0.02 * step).astype(jnp.bfloat16), m, v


def clipped(gradients, sum_of_squares, count):
    factor = jnp.minimum(1.0, 0.5 * lax.rsqrt(sum_of_squares / count + 1e-30))
    return [g * factor for g in gradients]


def stack(weights, h):
    return lax.scan(lambda h, w: (layer(h, w), None), h, weights)[0]


def reference(x, dy, w_gate, w_up, w_down, m_w_gate, m_w_up, m_w_down, v_w_gate, v_w_up, v_w_down):
    weights = dict(zip(NAMES, (w_gate, w_up, w_down), strict=True))

    def take(so_far, sequence):
        h, by_y = sequence
        _, back = jax.vjp(lambda w: stack(w, h), weights)
        return jax.tree.map(lambda total, term: total + term.astype(jnp.float32), so_far, back(by_y)[0]), None

    none_yet = {name: jnp.zeros(w.shape, jnp.float32) for name, w in weights.items()}
    by_weights, _ = lax.scan(take, none_yet, (x, dy))
    gradients = [by_weights[name].astype(jnp.bfloat16).astype(jnp.float32) for name in NAMES]
    gradients = clipped(gradients, sum(jnp.sum(g * g) for g in gradients), sum(g.size for g in gradients))
    new = [
        adamw(w.astype(jnp.float32), m, v, g)
        for w, m, v, g in zip((w_gate, w_up, w_down), (m_w_gate, m_w_up, m_w_down), (v_w_gate, v_w_up, v_w_down), gradients, strict=True)
    ]
    return tuple(one[which] for which in range(3) for one in new)
```

```python
import jax
import jax.numpy as jnp
from jax import lax
from jax.experimental import pallas as pl
from jax.experimental.pallas import tpu as pltpu
from jax.sharding import PartitionSpec as P


F32, BF16 = jnp.float32, jnp.bfloat16
ANY = pl.BlockSpec(memory_space=pl.ANY)


def call(kernel, grid, in_specs, out_specs, out_shape, flops, nbytes, scratch=(), aliases=None):
    return pl.pallas_call(
        kernel,
        grid=grid,
        in_specs=in_specs,
        out_specs=out_specs,
        out_shape=out_shape,
        scratch_shapes=scratch,
        input_output_aliases=aliases or {},
        cost_estimate=pl.CostEstimate(flops=flops, bytes_accessed=nbytes, transcendentals=0),
        compiler_params=pltpu.CompilerParams(
            dimension_semantics=("arbitrary",) * len(grid), vmem_limit_bytes=62 * 1024 * 1024
        ),
    )


def rows(bt, width):
    return pl.BlockSpec((bt, width), lambda i: (i, 0))


def cols(height, bt):
    return pl.BlockSpec((height, bt), lambda i: (0, i))


def whole(shape):
    return pl.BlockSpec(shape, lambda *i: (0,) * len(shape), pipeline_mode=pl.Buffered(1))


def sds(shape, dtype):
    return jax.ShapeDtypeStruct(shape, dtype)


def dot(a, b):
    return jnp.dot(a, b, preferred_element_type=F32)


def dot_nt(a, b):
    return lax.dot_general(a, b, (((1,), (1,)), ((), ())), preferred_element_type=F32)


def normed(h):
    wide = h.astype(F32)
    scale = lax.rsqrt(jnp.mean(wide * wide, -1, keepdims=True) + 1e-6)
    return (wide * scale).astype(BF16)


def pieces(f, parts=3):
    step = f // parts // 256 * 256
    return [(i * step, step if i < parts - 1 else f - i * step) for i in range(parts)]


def other_core():
    return lax.axis_index("rep") % 2


class Halves:
    def __init__(self, arrays, starts, count):
        self.arrays, self.starts, self.count = arrays, starts, count
        self.owners, self.height = arrays[0].shape[0], arrays[0].shape[1] // count

    def loads(self, refs, which, o, n, into, sem):
        core = other_core()
        out = []
        for part, start in enumerate(self.starts):
            end = start + self.arrays[2 * part].shape[2]
            low, high = max(o, start), min(o + n, end)
            if low >= high:
                continue
            for ref, side in ((refs[2 * part], core), (refs[2 * part + 1], 1 - core)):
                for owner in range(self.owners):
                    at = pl.multiple_of((2 * owner + side) * self.height, self.height)
                    out.append(
                        pltpu.make_async_copy(
                            ref.at[owner, pl.ds(which * self.height, self.height), pl.ds(low - start, high - low)],
                            into.at[pl.ds(at, self.height), pl.ds(low - o, high - low)],
                            sem.at[len(out)],
                        )
                    )
        return out

    def load_rows(self, refs, o, n, into, sem):
        core = other_core()
        out = []
        for block in range(2 * self.owners):
            start = block * self.height
            low, high = max(o, start), min(o + n, start + self.height)
            if low >= high:
                continue
            both = [
                pltpu.make_async_copy(
                    ref.at[block // 2, pl.ds(low - start, high - low), :], into.at[pl.ds(low - o, high - low), :], sem.at[len(out)]
                )
                for ref in refs
            ]
            pl.when(core == block % 2)(both[0].start)
            pl.when(core != block % 2)(both[1].start)
            out.append(both[0])
        return out


def begin(copies):
    for copy in copies:
        copy.start()
    return copies


def finish(copies):
    for copy in copies:
        copy.wait()


SEM = pltpu.SemaphoreType.DMA((16,))


def prepare(h, dy, bt=512):
    t, d = h.shape

    def kernel(h_ref, dy_ref, a_ref, at_ref, dyt_ref):
        a = normed(h_ref[...])
        a_ref[...] = a
        at_ref[...] = a.T
        dyt_ref[...] = dy_ref[...].T

    return call(
        kernel, (t // bt,), [rows(bt, d)] * 2, [rows(bt, d), cols(d, bt), cols(d, bt)],
        [sds((t, d), BF16), sds((d, t), BF16), sds((d, t), BF16)], 8 * t * d, 10 * t * d,
    )(h, dy)


def up(a, w, cut, bt=256):
    t, d = a.shape
    f = cut[-1][0] + cut[-1][1]
    k, m = len(cut), len(w.arrays)

    def kernel(a_ref, *refs):
        act_ref, *outs = refs[m : m + 1 + 2 * k]
        wg_ref, wu_ref, sem_g, sem_u = refs[m + 1 + 2 * k :]

        @pl.when(pl.program_id(0) == 0)
        def _():
            loads = begin(w.loads(refs[:m], 0, 0, f, wg_ref, sem_g)) + begin(w.loads(refs[:m], 1, 0, f, wu_ref, sem_u))
            finish(loads)

        a = a_ref[...]
        g, u = dot(a, wg_ref[...]), dot(a, wu_ref[...])
        for (o, n), g_ref, u_ref in zip(cut, outs[:k], outs[k:]):
            g_ref[...] = g[:, o : o + n]
            u_ref[...] = u[:, o : o + n]
        act_ref[...] = (g * jax.nn.sigmoid(g) * u).astype(BF16)

    return call(
        kernel, (t // bt,), [rows(bt, d)] + [ANY] * m,
        [rows(bt, f)] + [rows(bt, n) for _, n in cut] * 2,
        [sds((t, f), BF16)] + [sds((t, n), F32) for _, n in cut] * 2,
        4 * t * d * f, 10 * t * f, [pltpu.VMEM((d, f), BF16)] * 2 + [SEM] * 2,
    )(a, *w.arrays)


def down(act, w, h, bt=512):
    t, f = act.shape
    d = h.shape[1]

    def kernel(act_ref, mine, theirs, h_ref, o_ref, a_ref, at_ref, wd_ref, sem):
        @pl.when(pl.program_id(0) == 0)
        def _():
            finish(w.load_rows((mine, theirs), 0, f, wd_ref, sem))

        o = h_ref[...] + dot(act_ref[...], wd_ref[...]).astype(BF16)
        o_ref[...] = o
        a = normed(o)
        a_ref[...] = a
        at_ref[...] = a.T

    return call(
        kernel, (t // bt,), [rows(bt, f), ANY, ANY, rows(bt, d)], [rows(bt, d), rows(bt, d), cols(d, bt)],
        [sds((t, d), BF16), sds((t, d), BF16), sds((d, t), BF16)], 2 * t * d * f, 2 * t * f, [pltpu.VMEM((f, d), BF16), SEM],
    )(act, *w.arrays, h)


def gated_back(g, u, by):
    s = jax.nn.sigmoid(g)
    silu = g * s
    by = by.astype(BF16).astype(F32)
    return ((by * u) * (s * (1.0 + g * (1.0 - s)))).astype(BF16), (by * silu).astype(BF16), (silu * u).astype(BF16)


def last_piece(a, at, dy, dyt, w, w_down, o, n, so_far, bt=512):
    t, d = a.shape
    f = 2 * w_down.owners * w_down.height
    steps, m = t // bt, len(w.arrays)

    def kernel(a_ref, at_ref, dy_ref, dyt_ref, *rest):
        dg_ref, du_ref, up_ref, down_hbm, wg_ref, wu_ref, wd_ref, sum_g, sum_u, sum_d, flipped, sem_g, sem_u, sem = rest[-14:]
        i = pl.program_id(0)

        @pl.when(i == 0)
        def _():
            loads = begin(w.loads(rest[:m], 0, o, n, wg_ref, sem_g)) + begin(w.loads(rest[:m], 1, o, n, wu_ref, sem_u))
            loads += w_down.load_rows(rest[m : m + 2], o, n, wd_ref, sem)
            for total in (sum_g, sum_u, sum_d):
                total[...] = jnp.zeros_like(total)
            finish(loads)

        g, u = dot(a_ref[...], wg_ref[...]), dot(a_ref[...], wu_ref[...])
        dg_ref[...], du_ref[...], act = gated_back(g, u, dot_nt(dy_ref[...], wd_ref[...]))
        sum_d[...] += dot(dyt_ref[...], act)
        sum_g[...] += dot(at_ref[...], dg_ref[...])
        sum_u[...] += dot(at_ref[...], du_ref[...])

        @pl.when(i == steps - 1)
        def _():
            flipped[...] = sum_d[...].astype(BF16).T
            store = pltpu.make_async_copy(flipped, down_hbm.at[pl.ds(o, n), :], sem.at[0])
            store.start()
            up_ref[:, :n] = sum_g[...].astype(BF16)
            up_ref[:, n:] = sum_u[...].astype(BF16)
            store.wait()

    return call(
        kernel, (steps,), [rows(bt, d), cols(d, bt)] * 2 + [ANY] * (m + 2 + len(so_far)),
        [rows(bt, n), rows(bt, n), whole((d, 2 * n)), ANY],
        [sds((t, n), BF16), sds((t, n), BF16), sds((d, 2 * n), BF16), sds((f, d), BF16)],
        12 * t * d * n, 4 * t * n + 8 * t * d,
        [pltpu.VMEM((d, n), BF16)] * 2 + [pltpu.VMEM((n, d), BF16)] + [pltpu.VMEM((d, n), F32)] * 3
        + [pltpu.VMEM((n, d), BF16), SEM, SEM, SEM],
        aliases={6 + m: 3} if so_far else None,
    )(a, at, dy, dyt, *w.arrays, *w_down.arrays, *so_far)


def first_piece(at, g, u, by, w_down, o, bt=512):
    d, t = at.shape
    n = g.shape[1]
    steps = t // bt

    def kernel(at_ref, g_ref, u_ref, by_ref, mine, theirs, up_ref, wd_ref, sum_g, sum_u, sem):
        i = pl.program_id(0)

        @pl.when(i == 0)
        def _():
            loads = w_down.load_rows((mine, theirs), o, n, wd_ref, sem)
            for total in (sum_g, sum_u):
                total[...] = jnp.zeros_like(total)
            finish(loads)

        dg, du, _ = gated_back(g_ref[...], u_ref[...], dot_nt(by_ref[...], wd_ref[...]))
        sum_g[...] += dot(at_ref[...], dg)
        sum_u[...] += dot(at_ref[...], du)

        @pl.when(i == steps - 1)
        def _():
            up_ref[:, :n] = sum_g[...].astype(BF16)
            up_ref[:, n:] = sum_u[...].astype(BF16)

    return call(
        kernel, (steps,), [cols(d, bt), rows(bt, n), rows(bt, n), rows(bt, d), ANY, ANY], whole((d, 2 * n)),
        sds((d, 2 * n), BF16), 6 * t * d * n, 8 * t * n + 4 * t * d,
        [pltpu.VMEM((n, d), BF16)] + [pltpu.VMEM((d, n), F32)] * 2 + [SEM],
    )(at, g, u, by, *w_down.arrays)


def input_back(dgs, dus, w, h, dy, cut, bt=256):
    t, d = h.shape
    f = cut[-1][0] + cut[-1][1]
    k, m = len(cut), len(w.arrays)

    def kernel(*refs):
        h_ref, dy_ref, o_ref, ot_ref, wg_ref, wu_ref, sem_g, sem_u = refs[2 * k + m :]

        @pl.when(pl.program_id(0) == 0)
        def _():
            parts = refs[2 * k : 2 * k + m]
            finish(begin(w.loads(parts, 0, 0, f, wg_ref, sem_g)) + begin(w.loads(parts, 1, 0, f, wu_ref, sem_u)))

        by_g = sum(dot_nt(r[...], wg_ref[:, o : o + n]) for r, (o, n) in zip(refs[:k], cut))
        by_u = sum(dot_nt(r[...], wu_ref[:, o : o + n]) for r, (o, n) in zip(refs[k : 2 * k], cut))
        by = (by_g.astype(BF16) + by_u.astype(BF16)).astype(F32)
        wide = h_ref[...].astype(F32)
        scale = lax.rsqrt(jnp.mean(wide * wide, -1, keepdims=True) + 1e-6)
        along = jnp.mean(by * wide, -1, keepdims=True) * (scale * scale * scale)
        o = dy_ref[...] + (by * scale - wide * along).astype(BF16)
        o_ref[...] = o
        ot_ref[...] = o.T

    return call(
        kernel, (t // bt,), [rows(bt, n) for _, n in cut] * 2 + [ANY] * m + [rows(bt, d)] * 2,
        [rows(bt, d), cols(d, bt)], [sds((t, d), BF16), sds((d, t), BF16)],
        4 * t * d * f, 4 * t * f, [pltpu.VMEM((d, f), BF16)] * 2 + [SEM] * 2,
    )(*dgs, *dus, *w.arrays, h, dy)


def down_grad(byt, act, bn=640):
    d, t = byt.shape
    f = act.shape[1]

    def kernel(l_ref, r_ref, o_ref):
        o_ref[...] = dot(l_ref[...], r_ref[...]).astype(BF16).T

    return call(
        kernel, (f // bn,), [whole((d, t)), cols(t, bn)], rows(bn, d), sds((f, d), BF16),
        2 * t * d * f, 2 * t * f + 2 * t * d,
    )(byt, act)


def adamw(w, m, v, g):
    m = 0.9 * m + 0.1 * g
    v = 0.95 * v + 0.05 * g * g
    step = m * lax.rsqrt(v + 1e-8) + 0.1 * w
    return (w - 0.02 * step).astype(BF16), m, v


def update(ws, ms, vs, grads, factor, runs, br):
    layers, height, width = ws[0].shape
    k, count = len(ws), sum(len(g) for g in grads)
    first = [sum(len(g) for g in grads[:l]) for l in range(layers)]

    def kernel(*refs):
        factor_ref = refs[0]
        w_refs, m_refs, v_refs = (refs[1 + i * k : 1 + (i + 1) * k] for i in range(3))
        g_refs = refs[1 + 3 * k : 1 + 3 * k + count]
        outs = refs[1 + 3 * k + count :]
        scale = factor_ref[0, 0]
        for l in range(layers):

            @pl.when(pl.program_id(0) == l)
            def _():
                for i in range(k):
                    for array, source, to, n in runs[l][i]:
                        s = slice(to, to + n)
                        g = g_refs[first[l] + array][:, source : source + n].astype(F32) * scale
                        outs[i][0, :, s], outs[k + i][0, :, s], outs[2 * k + i][0, :, s] = adamw(
                            w_refs[i][0, :, s].astype(F32), m_refs[i][0, :, s], v_refs[i][0, :, s], g
                        )

    block = pl.BlockSpec((1, br, width), lambda l, i: (l, i, 0))
    steps = height // br

    def of(l):
        return lambda at, i: (jnp.where(at == l, i, jnp.where(at < l, 0, steps - 1)), 0)

    size = layers * height * width
    return call(
        kernel, (layers, steps),
        [pl.BlockSpec(memory_space=pltpu.SMEM)] + [block] * (3 * k)
        + [pl.BlockSpec((br, g.shape[1]), of(l)) for l in range(layers) for g in grads[l]],
        [block] * (3 * k),
        [sds(w.shape, BF16) for w in ws] + [sds(w.shape, F32) for w in ws] * 2,
        20 * k * size, 24 * k * size,
    )(factor, *ws, *ms, *vs, *(g for l in grads for g in l))


def solution(mesh):
    reps = mesh.shape["rep"]
    pairs = [(i, i ^ 1) for i in range(reps)]

    def step(x, dy, *arrays):
        weights, m, v = (arrays[i : i + 3] for i in (0, 3, 6))
        core = lax.axis_index("rep") % 2

        def fetched(shards, columns=slice(None)):
            halves = [lax.dynamic_slice_in_dim(w[:, columns], core * (w.shape[0] // 2), w.shape[0] // 2, 0) for w in shards]
            half = halves[0] if len(halves) == 1 else jnp.concatenate(halves)
            mine = lax.all_gather(half, "dp", axis=0, tiled=False)
            return [mine, lax.ppermute(mine, "rep", pairs)]

        def scattered(g):
            return lax.psum_scatter(g, "dp", scatter_dimension=0, tiled=True)

        def squares(gs):
            return sum(jnp.sum(g.astype(F32) ** 2) for g in gs)

        x, dy = x[0], dy[0]
        cut0, cut1 = pieces(weights[0].shape[2], 2), pieces(weights[0].shape[2], 3)
        k0 = len(cut0)
        edge = cut1[1][0]
        gu0 = Halves(fetched([weights[0][0], weights[1][0]]), [0], 2)
        d0 = Halves(fetched([weights[2][0]]), [0], 1)
        d1 = Halves(fetched([weights[2][1]]), [0], 1)
        first = fetched([weights[0][1], weights[1][1]], slice(0, edge))
        rest = fetched([weights[0][1], weights[1][1]], slice(edge, None))
        gu1 = Halves(first + rest, [0, edge], 2)

        a0, a0t, dyt = prepare(x, dy)
        act0, *gu = up(a0, gu0, cut0)
        h1, a1, a1t = down(act0, d0, x)
        dgs, dus, up1, so_far = [], [], [], []
        for o, n in cut1:
            w = Halves(first, [0], 2) if o + n <= edge else Halves(rest, [edge], 2)
            dg, du, g, so_far = last_piece(a1, a1t, dy, dyt, w, d1, o, n, so_far)
            so_far = [so_far]
            dgs.append(dg)
            dus.append(du)
            up1.append(scattered(g))
        down1 = scattered(so_far[0])
        by, byt = input_back(dgs, dus, gu1, h1, dy, cut1)
        down0 = scattered(down_grad(byt, act0))
        up0 = [scattered(first_piece(a0t, gu[j], gu[k0 + j], by, d0, o)) for j, (o, n) in enumerate(cut0)]

        total = lax.psum(squares(up1) + squares([down1]) + squares([down0]) + squares(up0), "dp")
        count = lax.psum(1, "dp") * sum(w.size for w in weights)
        factor = jnp.minimum(1.0, 0.5 * lax.rsqrt(total / count + 1e-30)).reshape(1, 1)
        runs = [[[(j, i * n, o, n) for j, (o, n) in enumerate(cut)] for i in range(2)] for cut in (cut0, cut1)]
        new_up = update(weights[:2], m[:2], v[:2], [up0, up1], factor, runs, weights[0].shape[1] // 4)
        width = weights[2].shape[2]
        whole_run = [[(0, 0, 0, width)]]
        new_down = update(weights[2:], m[2:], v[2:], [[down0], [down1]], factor, [whole_run] * 2, weights[2].shape[1] // 5)
        return tuple(o for i in range(3) for o in (new_up[2 * i], new_up[2 * i + 1], new_down[i]))

    states, cut = P(("rep", "dp"), None, None), P(None, "dp", None)
    return jax.shard_map(
        step,
        mesh=mesh,
        in_specs=(states, states) + (cut,) * 9,
        out_specs=(P("rep", "dp", None),) * 9,
        check_vma=False,
    )
```

```python
import jax
import jax.numpy as jnp
from jax import lax
from jax.experimental import pallas as pl
from jax.experimental.pallas import tpu as pltpu
from jax.sharding import PartitionSpec as P


F32, BF16 = jnp.float32, jnp.bfloat16
MIB = 62
ANY = pl.BlockSpec(memory_space=pl.ANY)


def call(kernel, grid, in_specs, out_specs, out_shape, flops, nbytes, scratch=(), aliases=None, mib=62):
    return pl.pallas_call(
        kernel,
        grid=grid,
        in_specs=in_specs,
        out_specs=out_specs,
        out_shape=out_shape,
        scratch_shapes=scratch,
        input_output_aliases=aliases or {},
        cost_estimate=pl.CostEstimate(flops=flops, bytes_accessed=nbytes, transcendentals=0),
        compiler_params=pltpu.CompilerParams(
            dimension_semantics=("arbitrary",) * len(grid), vmem_limit_bytes=mib * 1024 * 1024
        ),
    )


def rows(bt, width):
    return pl.BlockSpec((bt, width), lambda i: (i, 0))


def cols(height, bt):
    return pl.BlockSpec((height, bt), lambda i: (0, i))


def whole(shape):
    return pl.BlockSpec(shape, lambda *i: (0,) * len(shape), pipeline_mode=pl.Buffered(1))


def sds(shape, dtype):
    return jax.ShapeDtypeStruct(shape, dtype)


def dot(a, b):
    return jnp.dot(a, b, preferred_element_type=F32)


def dot_nt(a, b):
    return lax.dot_general(a, b, (((1,), (1,)), ((), ())), preferred_element_type=F32)


def dot_tn(a, b):
    return lax.dot_general(a, b, (((0,), (0,)), ((), ())), preferred_element_type=F32)


def normed(h):
    wide = h.astype(F32)
    scale = lax.rsqrt(jnp.mean(wide * wide, -1, keepdims=True) + 1e-6)
    return (wide * scale).astype(BF16)


def pieces(f, shares):
    ends = [f * sum(shares[:i]) // sum(shares) for i in range(len(shares) + 1)]
    return [(low, high - low) for low, high in zip(ends, ends[1:])]


def other_core():
    return lax.axis_index("rep") % 2


class Halves:
    def __init__(self, arrays, starts, height, bases=None):
        self.arrays, self.starts, self.height = arrays, starts, height
        self.owners, self.bases = arrays[0].shape[0], bases or [0] * len(starts)

    def loads(self, refs, which, o, n, into, sem):
        core = other_core()
        out = []
        for part, start in enumerate(self.starts):
            end = start + self.arrays[2 * part].shape[2]
            low, high = max(o, start), min(o + n, end)
            if low >= high:
                continue
            for ref, side in ((refs[2 * part], core), (refs[2 * part + 1], 1 - core)):
                for owner in range(self.owners):
                    at = pl.multiple_of((2 * owner + side) * self.height, self.height)
                    out.append(
                        pltpu.make_async_copy(
                            ref.at[owner, pl.ds(self.bases[part] + which * self.height, self.height), pl.ds(low - start, high - low)],
                            into.at[pl.ds(at, self.height), pl.ds(low - o, high - low)],
                            sem.at[len(out)],
                        )
                    )
        return out

    def load_rows(self, refs, o, n, into, sem):
        core = other_core()
        out = []
        for block in range(2 * self.owners):
            start = block * self.height
            low, high = max(o, start), min(o + n, start + self.height)
            if low >= high:
                continue
            both = [
                pltpu.make_async_copy(
                    ref.at[block // 2, pl.ds(low - start, high - low), :], into.at[pl.ds(low - o, high - low), :], sem.at[len(out)]
                )
                for ref in refs
            ]
            pl.when(core == block % 2)(both[0].start)
            pl.when(core != block % 2)(both[1].start)
            out.append(both[0])
        return out


def begin(copies):
    for copy in copies:
        copy.start()
    return copies


def finish(copies):
    for copy in copies:
        copy.wait()


SEM = pltpu.SemaphoreType.DMA((16,))


def halve(wanted):
    entries = [e for some in wanted for e in some]
    shapes = [(sum(w.shape[1] // 2 for w, *_ in some), some[0][3]) for some in wanted]

    def kernel(*refs):
        ins, outs, sem = refs[: len(entries)], refs[len(entries) : -1], refs[-1]
        copies = []
        for some, out in zip(wanted, outs):
            at = 0
            for w, layer, o, n in some:
                h = w.shape[1] // 2
                source = ins[len(copies)].at[layer, pl.ds(pl.multiple_of(other_core() * h, h), h), pl.ds(o, n)]
                copies.append(pltpu.make_async_copy(source, out.at[pl.ds(at, h), :], sem.at[len(copies)]))
                at += h
        finish(begin(copies))

    return call(
        kernel, (1,), [ANY] * len(entries), [whole(s) for s in shapes], [sds(s, BF16) for s in shapes],
        1000000, 4 * sum(a * b for a, b in shapes), [SEM],
    )(*(e[0] for e in entries))


def prepare(h, dy, bt=512):
    t, d = h.shape

    def kernel(h_ref, dy_ref, a_ref, at_ref, dyt_ref):
        a = normed(h_ref[...])
        a_ref[...] = a
        at_ref[...] = a.T
        dyt_ref[...] = dy_ref[...].T

    return call(
        kernel, (t // bt,), [rows(bt, d)] * 2, [rows(bt, d), cols(d, bt), cols(d, bt)],
        [sds((t, d), BF16), sds((d, t), BF16), sds((d, t), BF16)], 8 * t * d, 10 * t * d,
    )(h, dy)


def up(a, w, o, n, bt=256):
    t, d = a.shape
    m = len(w.arrays)

    def kernel(a_ref, *refs):
        act_ref, g_ref, u_ref, wg_ref, wu_ref, sem_g, sem_u = refs[m:]

        @pl.when(pl.program_id(0) == 0)
        def _():
            finish(begin(w.loads(refs[:m], 0, o, n, wg_ref, sem_g)) + begin(w.loads(refs[:m], 1, o, n, wu_ref, sem_u)))

        g, u = dot(a_ref[...], wg_ref[...]), dot(a_ref[...], wu_ref[...])
        g_ref[...] = g
        u_ref[...] = u
        act_ref[...] = (g * jax.nn.sigmoid(g) * u).astype(BF16)

    return call(
        kernel, (t // bt,), [rows(bt, d)] + [ANY] * m, [rows(bt, n)] * 3,
        [sds((t, n), BF16), sds((t, n), F32), sds((t, n), F32)],
        4 * t * d * n, 10 * t * n, [pltpu.VMEM((d, n), BF16)] * 2 + [SEM] * 2,
    )(a, *w.arrays)


def down(acts, w, h, cut, bt=512):
    t, d = h.shape
    f, k = cut[-1][0] + cut[-1][1], len(cut)

    def kernel(*refs):
        mine, theirs, h_ref, o_ref, a_ref, at_ref, wd_ref, sem = refs[k:]

        @pl.when(pl.program_id(0) == 0)
        def _():
            finish(w.load_rows((mine, theirs), 0, f, wd_ref, sem))

        total = sum(dot(r[...], wd_ref[o : o + n, :]) for r, (o, n) in zip(refs[:k], cut))
        o = h_ref[...] + total.astype(BF16)
        o_ref[...] = o
        a = normed(o)
        a_ref[...] = a
        at_ref[...] = a.T

    return call(
        kernel, (t // bt,), [rows(bt, n) for _, n in cut] + [ANY, ANY, rows(bt, d)], [rows(bt, d), rows(bt, d), cols(d, bt)],
        [sds((t, d), BF16), sds((t, d), BF16), sds((d, t), BF16)], 2 * t * d * f, 2 * t * f, [pltpu.VMEM((f, d), BF16), SEM],
    )(*acts, *w.arrays, h)


def gated_back(g, u, by):
    s = jax.nn.sigmoid(g)
    silu = g * s
    by = by.astype(BF16).astype(F32)
    return ((by * u) * (s * (1.0 + g * (1.0 - s)))).astype(BF16), (by * silu).astype(BF16), (silu * u).astype(BF16)


def last_piece(a, at, dy, dyt, w, w_down, o, n, so_far, bt=512):
    t, d = a.shape
    f = 2 * w_down.owners * w_down.height
    steps, m = t // bt, len(w.arrays)

    def kernel(a_ref, at_ref, dy_ref, dyt_ref, *rest):
        dg_ref, du_ref, up_ref, down_hbm, wg_ref, wu_ref, wd_ref, sum_g, sum_u, sum_d, flipped, sem_g, sem_u, sem = rest[-14:]
        i = pl.program_id(0)

        @pl.when(i == 0)
        def _():
            loads = begin(w.loads(rest[:m], 0, o, n, wg_ref, sem_g)) + begin(w.loads(rest[:m], 1, o, n, wu_ref, sem_u))
            loads += w_down.load_rows(rest[m : m + 2], o, n, wd_ref, sem)
            for total in (sum_g, sum_u, sum_d):
                total[...] = jnp.zeros_like(total)
            finish(loads)

        g, u = dot(a_ref[...], wg_ref[...]), dot(a_ref[...], wu_ref[...])
        dg_ref[...], du_ref[...], act = gated_back(g, u, dot_nt(dy_ref[...], wd_ref[...]))
        sum_d[...] += dot(dyt_ref[...], act)
        sum_g[...] += dot(at_ref[...], dg_ref[...])
        sum_u[...] += dot(at_ref[...], du_ref[...])

        @pl.when(i == steps - 1)
        def _():
            flipped[...] = sum_d[...].astype(BF16).T
            store = pltpu.make_async_copy(flipped, down_hbm.at[pl.ds(o, n), :], sem.at[0])
            store.start()
            up_ref[:, :n] = sum_g[...].astype(BF16)
            up_ref[:, n:] = sum_u[...].astype(BF16)
            store.wait()

    return call(
        kernel, (steps,), [rows(bt, d), cols(d, bt)] * 2 + [ANY] * (m + 2 + len(so_far)),
        [rows(bt, n), rows(bt, n), whole((d, 2 * n)), ANY],
        [sds((t, n), BF16), sds((t, n), BF16), sds((d, 2 * n), BF16), sds((f, d), BF16)],
        12 * t * d * n, 4 * t * n + 8 * t * d,
        [pltpu.VMEM((d, n), BF16)] * 2 + [pltpu.VMEM((n, d), BF16)] + [pltpu.VMEM((d, n), F32)] * 3
        + [pltpu.VMEM((n, d), BF16), SEM, SEM, SEM],
        aliases={6 + m: 3} if so_far else None,
    )(a, at, dy, dyt, *w.arrays, *w_down.arrays, *so_far)


def first_piece(at, g, u, by, w_down, o, bt=512):
    d, t = at.shape
    n = g.shape[1]
    steps = t // bt

    def kernel(at_ref, g_ref, u_ref, by_ref, mine, theirs, up_ref, wd_ref, sum_g, sum_u, sem):
        i = pl.program_id(0)

        @pl.when(i == 0)
        def _():
            loads = w_down.load_rows((mine, theirs), o, n, wd_ref, sem)
            for total in (sum_g, sum_u):
                total[...] = jnp.zeros_like(total)
            finish(loads)

        dg, du, _ = gated_back(g_ref[...], u_ref[...], dot_nt(by_ref[...], wd_ref[...]))
        sum_g[...] += dot(at_ref[...], dg)
        sum_u[...] += dot(at_ref[...], du)

        @pl.when(i == steps - 1)
        def _():
            up_ref[:, :n] = sum_g[...].astype(BF16)
            up_ref[:, n:] = sum_u[...].astype(BF16)

    return call(
        kernel, (steps,), [cols(d, bt), rows(bt, n), rows(bt, n), rows(bt, d), ANY, ANY], whole((d, 2 * n)),
        sds((d, 2 * n), BF16), 6 * t * d * n, 8 * t * n + 4 * t * d,
        [pltpu.VMEM((n, d), BF16)] + [pltpu.VMEM((d, n), F32)] * 2 + [SEM],
    )(at, g, u, by, *w_down.arrays)


def input_back(dgs, dus, w, h, dy, cut, bt=256):
    t, d = h.shape
    f = cut[-1][0] + cut[-1][1]
    k, m = len(cut), len(w.arrays)

    def kernel(*refs):
        h_ref, dy_ref, o_ref, wg_ref, wu_ref, sem_g, sem_u = refs[2 * k + m :]

        @pl.when(pl.program_id(0) == 0)
        def _():
            parts = refs[2 * k : 2 * k + m]
            finish(begin(w.loads(parts, 0, 0, f, wg_ref, sem_g)) + begin(w.loads(parts, 1, 0, f, wu_ref, sem_u)))

        by_g = sum(dot_nt(r[...], wg_ref[:, o : o + n]) for r, (o, n) in zip(refs[:k], cut))
        by_u = sum(dot_nt(r[...], wu_ref[:, o : o + n]) for r, (o, n) in zip(refs[k : 2 * k], cut))
        by = (by_g.astype(BF16) + by_u.astype(BF16)).astype(F32)
        wide = h_ref[...].astype(F32)
        scale = lax.rsqrt(jnp.mean(wide * wide, -1, keepdims=True) + 1e-6)
        along = jnp.mean(by * wide, -1, keepdims=True) * (scale * scale * scale)
        o_ref[...] = dy_ref[...] + (by * scale - wide * along).astype(BF16)

    return call(
        kernel, (t // bt,), [rows(bt, n) for _, n in cut] * 2 + [ANY] * m + [rows(bt, d)] * 2,
        rows(bt, d), sds((t, d), BF16), 4 * t * d * f, 4 * t * f, [pltpu.VMEM((d, f), BF16)] * 2 + [SEM] * 2,
    )(*dgs, *dus, *w.arrays, h, dy)


def down_grad(by, acts, bn=640):
    t, d = by.shape
    counts = [a.shape[1] // bn for a in acts]
    firsts = [sum(counts[:i]) for i in range(len(acts))]
    steps = sum(counts)

    def kernel(by_ref, *refs):
        o_ref = refs[-1]
        for r, first, count in zip(refs, firsts, counts):

            @pl.when((pl.program_id(0) >= first) & (pl.program_id(0) < first + count))
            def _():
                o_ref[...] = dot_tn(r[...], by_ref[...]).astype(BF16)

    def of(first, count):
        return lambda i: (0, jnp.clip(i - first, 0, count - 1))

    return call(
        kernel, (steps,), [whole((t, d))] + [pl.BlockSpec((t, bn), of(f, c)) for f, c in zip(firsts, counts)],
        rows(bn, d), sds((steps * bn, d), BF16), 2 * t * d * steps * bn, 2 * t * steps * bn + 2 * t * d,
    )(by, *acts)


def adamw(w, m, v, g):
    m = 0.9 * m + 0.1 * g
    v = 0.95 * v + 0.05 * g * g
    step = m * lax.rsqrt(v + 1e-8) + 0.1 * w
    return (w - 0.02 * step).astype(BF16), m, v


def update(ws, ms, vs, grads, factor, runs, br):
    layers, height, width = ws[0].shape
    k, count = len(ws), sum(len(g) for g in grads)
    first = [sum(len(g) for g in grads[:l]) for l in range(layers)]

    def kernel(*refs):
        factor_ref = refs[0]
        w_refs, m_refs, v_refs = (refs[1 + i * k : 1 + (i + 1) * k] for i in range(3))
        g_refs = refs[1 + 3 * k : 1 + 3 * k + count]
        outs = refs[1 + 3 * k + count :]
        scale = factor_ref[0, 0]
        for l in range(layers):

            @pl.when(pl.program_id(0) == l)
            def _():
                for i in range(k):
                    for array, source, to, n in runs[l][i]:
                        s = slice(to, to + n)
                        g = g_refs[first[l] + array][:, source : source + n].astype(F32) * scale
                        outs[i][0, :, s], outs[k + i][0, :, s], outs[2 * k + i][0, :, s] = adamw(
                            w_refs[i][0, :, s].astype(F32), m_refs[i][0, :, s], v_refs[i][0, :, s], g
                        )

    block = pl.BlockSpec((1, br, width), lambda l, i: (l, i, 0))
    steps = height // br

    def of(l):
        return lambda at, i: (jnp.where(at == l, i, jnp.where(at < l, 0, steps - 1)), 0)

    size = layers * height * width
    return call(
        kernel, (layers, steps),
        [pl.BlockSpec(memory_space=pltpu.SMEM)] + [block] * (3 * k)
        + [pl.BlockSpec((br, g.shape[1]), of(l)) for l in range(layers) for g in grads[l]],
        [block] * (3 * k),
        [sds(w.shape, BF16) for w in ws] + [sds(w.shape, F32) for w in ws] * 2,
        20 * k * size, 24 * k * size, mib=MIB,
    )(factor, *ws, *ms, *vs, *(g for l in grads for g in l))


def solution(mesh):
    reps = mesh.shape["rep"]
    pairs = [(i, i ^ 1) for i in range(reps)]

    def step(x, dy, *arrays):
        weights, m, v = (arrays[i : i + 3] for i in (0, 3, 6))

        def fetched(half):
            mine = lax.all_gather(half, "dp", axis=0, tiled=False)
            return [mine, lax.ppermute(mine, "rep", pairs)]

        def scattered(g):
            return lax.psum_scatter(g, "dp", scatter_dimension=0, tiled=True)

        def squares(gs):
            return sum(jnp.sum(g.astype(F32) ** 2) for g in gs)

        x, dy = x[0], dy[0]
        f = weights[0].shape[2]
        cut0, cut1 = pieces(f, (2, 3)), pieces(f, (8, 10, 7))
        split, edge = cut0[1][0], cut1[1][0]
        gate, up_, down_ = weights
        d = down_.shape[2]
        up_height, down_height = gate.shape[1] // 2, down_.shape[1] // 2
        (half,) = halve([[(gate, 0, 0, split), (up_, 0, 0, split)]])
        gu0a = fetched(half)
        halves = halve(
            [
                [(gate, 0, split, f - split), (up_, 0, split, f - split)],
                [(down_, 0, 0, d)],
                [(down_, 1, 0, d), (gate, 1, 0, edge), (up_, 1, 0, edge)],
                [(gate, 1, edge, f - edge), (up_, 1, edge, f - edge)],
            ]
        )
        gu0b = fetched(halves[0])
        d0 = Halves(fetched(halves[1]), [0], down_height)
        first, rest = fetched(halves[2]), fetched(halves[3])
        d1 = Halves(first, [0], down_height)
        gu1 = Halves(first + rest, [0, edge], up_height, [down_height, 0])

        a0, a0t, dyt = prepare(x, dy)
        act0a, g0a, u0a = up(a0, Halves(gu0a, [0], up_height), *cut0[0])
        act0b, g0b, u0b = up(a0, Halves(gu0b, [split], up_height), *cut0[1])
        h1, a1, a1t = down([act0a, act0b], d0, x, cut0)
        dgs, dus, up1, so_far = [], [], [], []
        for o, n in cut1:
            w = Halves(first, [0], up_height, [down_height]) if o + n <= edge else Halves(rest, [edge], up_height)
            dg, du, g, so_far = last_piece(a1, a1t, dy, dyt, w, d1, o, n, so_far)
            so_far = [so_far]
            dgs.append(dg)
            dus.append(du)
            up1.append(scattered(g))
        down1 = scattered(so_far[0])
        by = input_back(dgs, dus, gu1, h1, dy, cut1)
        down0 = scattered(down_grad(by, [act0a, act0b]))
        up0 = [
            scattered(first_piece(a0t, g0a, u0a, by, d0, cut0[0][0])),
            scattered(first_piece(a0t, g0b, u0b, by, d0, cut0[1][0], 256)),
        ]

        total = lax.psum(squares(up1) + squares([down1]) + squares([down0]) + squares(up0), "dp")
        count = lax.psum(1, "dp") * sum(w.size for w in weights)
        factor = jnp.minimum(1.0, 0.5 * lax.rsqrt(total / count + 1e-30)).reshape(1, 1)
        runs = [[[(j, i * n, o, n) for j, (o, n) in enumerate(cut)] for i in range(2)] for cut in (cut0, cut1)]
        new_up = update(weights[:2], m[:2], v[:2], [up0, up1], factor, runs, weights[0].shape[1] // 4)
        width = weights[2].shape[2]
        whole_run = [[(0, 0, 0, width)]]
        new_down = update(weights[2:], m[2:], v[2:], [[down0], [down1]], factor, [whole_run] * 2, weights[2].shape[1] // 5)
        return tuple(o for i in range(3) for o in (new_up[2 * i], new_up[2 * i + 1], new_down[i]))

    states, cut = P(("rep", "dp"), None, None), P(None, "dp", None)
    return jax.shard_map(
        step,
        mesh=mesh,
        in_specs=(states, states) + (cut,) * 9,
        out_specs=(P("rep", "dp", None),) * 9,
        check_vma=False,
    )
```
